32 devices in a mesh: dp: 4 (over y, core), expert: 2 (over x), group: 4 (over z).
Axes of the slice: x: 2, y: 2, z: 4, core: 2. Of those that a mesh axis runs over, the one named last changes fastest.
Arguments:
- tokens: bfloat16 [256, 7168], P(('dp', 'group')), may hold values from -6 to 6
- expert_ids: int32 [256, 8], P(('dp', 'group')), may hold values from 0 to 255, all different within a row; in each aligned block of 16 rows (0 to 15, 16 to 31, ...) at most 2 rows name the same one
- gate_values: bfloat16 [256, 8], P(('dp', 'group')), may hold values from 0.099609375 to 1
- gate_up: bfloat16 [2, 7168, 2, 2048], P('expert', None, None, 'group'), may hold values from -0.0625 to 0.0625
- down_weight: bfloat16 [2, 2048, 7168], P('expert', 'group'), may hold values from -0.125 to 0.125
- shared_gate_up: bfloat16 [7168, 2, 2048], P('expert', None, 'group'), may hold values from -0.0625 to 0.0625
- shared_down: bfloat16 [2048, 7168], P('group', 'expert'), may hold values from -0.125 to 0.125
Outputs:
- mixed: bfloat16 [256, 7168], P(('dp', 'group'), 'expert')
The draws below stay inside these ranges and needn't reach their ends.
Inputs may be any that keep to these rules, and one draw needn't show every extreme that they name: `expert_ids`: each row names 8 different routed experts. In each aligned block of 16 rows (the rows of one device) no expert is named by more than 2 rows, and in some blocks one is named by exactly 2 rows.
All inputs are finite; a program needn't handle non-finite values.
Results may differ from the reference program's by a relative error of at most 0.028.
Values may be sent and summed in bfloat16 or wider, within the bound.
A program may use at most 128 MiB of HBM per device.

```python
import math
import jax
import jax.numpy as jnp
import numpy as np

D = 7168
FF = 2048
ROUTED = 256
TOPK = 8
TOK_DEV = 16
CAP = 2
SLOTS = 2
FF_DEV = 512
TOKENS = 256
N_GROUP = 4


def block_levels(rng, dims, pieces, smallest, top_value):
    gain, own = 1.0, jax.random.fold_in(rng, 6)
    for position, parts in pieces:
        heights = jnp.exp(jax.random.uniform(jax.random.fold_in(own, position), (parts,), jnp.float32, smallest / len(pieces), top_value / len(pieces)))
        gain = gain * jnp.repeat(heights, dims[position] // parts).reshape([-1 if axis == position else 1 for axis in range(len(dims))])
    return gain


def routed_block(stream_key, own, number, rows, number_of, top, limit, skew):
    ranking = jax.random.permutation(stream_key, number_of)
    crowded, common = portions_of(number_of, rows * top, limit, skew, True), portions_of(number_of, rows * top, limit, skew, False)
    places = jnp.arange(number_of)

    def named(tallies, rotation):
        used = int((tallies > 0).sum())
        fixed = max(1, used // 4)
        moved = fixed + (places - fixed + rotation * (used - fixed)) % max(1, number_of - fixed)
        return jnp.zeros((number_of,), jnp.int32).at[ranking[jnp.where(places < fixed, places, moved)]].set(jnp.asarray(tallies, jnp.int32))

    tallies = jnp.where(number % 4 == 0, named(crowded, number // 4), named(common, number - number // 4 - 1))
    mixed = jax.random.permutation(jax.random.fold_in(own, 3), number_of)
    source_of, sink = mixed[0:number_of // 2 * 2:2], mixed[1:number_of // 2 * 2:2]
    room = jnp.minimum(tallies[source_of] - 1, limit - tallies[sink]) // 2
    room = jnp.where((source_of == ranking[0]) | (sink == ranking[0]) | (tallies[sink] == 0), 0, jnp.maximum(room, 0))
    moved = jax.random.randint(jax.random.fold_in(own, 4), (number_of // 2,), 0, 1 << 20) % (room + 1)
    tallies = tallies.at[source_of].add(-moved).at[sink].add(moved)
    members = jnp.searchsorted(jnp.cumsum(tallies), jnp.arange(rows * top), side="right").astype(jnp.int32)
    table = members.reshape(top, rows).T
    table = table[jax.random.permutation(jax.random.fold_in(own, 1), rows)]
    rotation = jax.random.randint(jax.random.fold_in(own, 2), (rows, 1), 0, top)
    return jnp.take_along_axis(table, (jnp.arange(top)[None, :] + rotation) % top, axis=1)


def portions_of(amount, total, reach, lean, full):
    weights = [(1 << 20) // math.isqrt(rank ** lean) + 1 for rank in range(1, amount + 1)]
    largest = reach if full else min(reach, max(-(-total // amount), total * weights[0] // sum(weights)))
    least = 1 if total - largest >= amount - 1 else 0
    counts, rest = [largest] + [least] * (amount - 1), total - largest - least * (amount - 1)
    while rest > 0:
        movable = [i for i in range(1, amount) if counts[i] < largest] or [i for i in range(1, amount) if counts[i] < reach]
        pool, left = sum([weights[i] for i in movable]), rest
        for i in movable:
            more = min(reach - counts[i], max(1, left * weights[i] // pool), rest)
            counts[i] = counts[i] + more
            rest = rest - more
    return np.array(counts)


def centred(key, extent, width, bound, pieces=(), dtype=jnp.bfloat16):
    result = jax.random.normal(key, extent, jnp.float32) * width
    if len(pieces) > 0:
        result = block_levels(key, extent, pieces, -0.22, 0.18) * result
    return jnp.clip(result, min=-bound, max=bound).astype(dtype)


def setup_inputs(seed: int = 0) -> dict:
    streams_of = jax.random.split(jax.random.key(seed), 8)
    tokens = centred(streams_of[0], (TOKENS, D), 1.0, 6.0, ((0, 16),))
    expert_ids_keys = jax.random.split(jax.random.fold_in(streams_of[1], 1), TOKENS // TOK_DEV)
    expert_ids_turns = jax.random.permutation(jax.random.fold_in(streams_of[1], 3), TOKENS // TOK_DEV)
    expert_ids = jax.vmap(lambda own, number: routed_block(jax.random.fold_in(streams_of[1], 2), own, number, TOK_DEV, ROUTED, TOPK, CAP, 2))(expert_ids_keys, expert_ids_turns).reshape((TOKENS, TOPK))
    gate_values = jnp.clip(jnp.exp(math.log(1.0) - 2.306499 * jax.random.uniform(streams_of[2], (TOKENS, TOPK), jnp.float32) ** block_levels(streams_of[2], (TOKENS, TOPK), ((0, 16),), -0.2, 0.2)), 0.099609375, 1.0).astype(jnp.bfloat16)
    gate_up = centred(streams_of[3], (SLOTS, D, 2, FF), D ** -0.5, 0.0625, ((0, 2), (3, 4)))
    down_weight = centred(streams_of[4], (SLOTS, FF, D), FF ** -0.5, 0.125, ((0, 2), (1, 4)))
    shared_gate_up = centred(streams_of[5], (D, 2, FF), D ** -0.5, 0.0625, ((0, 2), (2, 4)))
    shared_down = centred(streams_of[6], (FF, D), FF ** -0.5, 0.125, ((0, 4), (1, 2)))
    return {"tokens": tokens, "expert_ids": expert_ids, "gate_values": gate_values, "gate_up": gate_up, "down_weight": down_weight, "shared_gate_up": shared_gate_up, "shared_down": shared_down}


def reference(tokens, expert_ids, gate_values, gate_up, down_weight, shared_gate_up, shared_down):
    accumulated = jnp.zeros((TOKENS, D), jnp.float32)
    for slot_index in range(SLOTS):
        chosen = expert_ids == slot_index
        slot_weight = jnp.sum(jnp.where(chosen, gate_values.astype(jnp.float32), jnp.float32(0.0)), axis=1)
        gate_part = jnp.dot(tokens, gate_up[slot_index, :, 0, :], preferred_element_type=jnp.float32)
        up_part = jnp.dot(tokens, gate_up[slot_index, :, 1, :], preferred_element_type=jnp.float32)
        hidden = (jax.nn.silu(gate_part) * up_part).astype(jnp.bfloat16)
        for block_index in range(N_GROUP):
            first_unit = block_index * FF_DEV
            product = jnp.dot(hidden[:, first_unit:first_unit + FF_DEV],
                              down_weight[slot_index, first_unit:first_unit + FF_DEV, :],
                              preferred_element_type=jnp.float32)
            slot_term = (product * slot_weight[:, None]).astype(jnp.bfloat16)
            accumulated = accumulated + slot_term.astype(jnp.float32)
    shared_gate = jnp.dot(tokens, shared_gate_up[:, 0, :], preferred_element_type=jnp.float32)
    shared_up = jnp.dot(tokens, shared_gate_up[:, 1, :], preferred_element_type=jnp.float32)
    shared_hidden = (jax.nn.silu(shared_gate) * shared_up).astype(jnp.bfloat16)
    for block_index in range(N_GROUP):
        first_unit = block_index * FF_DEV
        shared_term = jnp.dot(shared_hidden[:, first_unit:first_unit + FF_DEV],
                              shared_down[first_unit:first_unit + FF_DEV, :],
                              preferred_element_type=jnp.float32).astype(jnp.bfloat16)
        accumulated = accumulated + shared_term.astype(jnp.float32)
    return accumulated.astype(jnp.bfloat16)
```

```python
import functools

import jax
import jax.numpy as jnp
from jax import lax
from jax.experimental import pallas as pl
from jax.experimental.pallas import tpu as pltpu
from jax.sharding import PartitionSpec as P

MESH = pl.DeviceIdType.MESH
BF16, F32 = jnp.bfloat16, jnp.float32
CAP = 2
LANES = 128
DEPTH = 1792


def nearest_first(count):
    order = [0]
    for distance in range(1, count // 2 + 1):
        for candidate in (distance, count - distance):
            if candidate not in order:
                order.append(candidate)
    return order


def silu(value):
    return value / (1.0 + jnp.exp(-value))


def kernel(
    n_expert, n_group, batch,
    tokens, ids, gates, gate_up, down, shared_gate_up, shared_down,
    out,
    w_routed, w_down, w_shared, w_shared_down,
    x_all, x_shared, rows_all, x_routed,
    pre_own, pre_out, pre_in, term_out, term_in, routed_out, routed_in,
    routed_w_sem, down_w_sem, shared_w_sem, shared_down_w_sem, own_sem,
    x_send, x_recv, rows_send, rows_recv, pre_send, pre_recv,
    term_send, term_recv, routed_send, routed_recv,
):
    me_e, me_g = lax.axis_index("expert"), lax.axis_index("group")
    n_tokens, width = tokens.shape
    columns = x_all.shape[2]
    units = w_shared_down.shape[0]
    tiles = units // LANES
    pair = 2 if tiles % 2 == 0 else 1
    order = nearest_first(n_group)
    batches = [order[i : i + batch] for i in range(0, n_group, batch)]
    n_rows = batch * n_tokens

    def expert_at(distance):
        return lax.rem(me_e + n_expert + distance, n_expert)

    def group_at(distance):
        return lax.rem(me_g + n_group + distance, n_group)

    def weight_copies(source, target, sem):
        depth = min(DEPTH, source.shape[0])
        groups = []
        for n in range(source.shape[0] // depth):
            rows = pl.ds(n * depth, depth)
            groups.append([
                pltpu.make_async_copy(
                    source.at[rows, pl.ds(c * LANES, LANES)], target.at[c, rows], sem.at[n, c]
                )
                for c in range(tiles)
            ])
        return groups

    shared_groups = weight_copies(
        shared_gate_up.reshape(2 * columns, units), w_shared, shared_w_sem
    )
    routed_groups = weight_copies(gate_up.reshape(2 * width, units), w_routed, routed_w_sem)
    part = units // 4
    shared_down_copies = [
        pltpu.make_async_copy(
            shared_down.at[pl.ds(i * part, part)], w_shared_down.at[pl.ds(i * part, part)],
            shared_down_w_sem.at[i],
        )
        for i in range(4)
    ]
    down_copies = [
        pltpu.make_async_copy(
            down.at[0, :, pl.ds(pl.multiple_of(expert_at(-d) * columns, LANES), columns)],
            w_down.at[d],
            down_w_sem.at[d],
        )
        for d in range(n_expert)
    ]
    own_columns = pl.ds(pl.multiple_of(me_e * columns, LANES), columns)
    own_copy = pltpu.make_async_copy(tokens.at[:, own_columns], x_all.at[0], own_sem)
    own_copy.start()
    for group in shared_groups:
        for copy in group:
            copy.start()
    for copy in shared_down_copies:
        copy.start()
    for group in routed_groups:
        for copy in group:
            copy.start()
    for copy in down_copies:
        copy.start()

    barrier = pltpu.get_barrier_semaphore()
    for d in range(n_expert):
        for s in range(n_group):
            if d or s:
                pl.semaphore_signal(
                    barrier, inc=1,
                    device_id={"expert": expert_at(d), "group": group_at(s)},
                    device_id_type=MESH,
                )

    before = (
        lax.broadcasted_iota(jnp.int32, (n_tokens, n_tokens), 0)
        < lax.broadcasted_iota(jnp.int32, (n_tokens, n_tokens), 1)
    ).astype(BF16)
    ranks = lax.broadcasted_iota(jnp.int32, (8, n_tokens), 0).astype(F32)

    def picked_by(expert):
        chosen = ids[...] == expert
        named = jnp.sum(jnp.where(chosen, 1.0, 0.0), axis=0, keepdims=True)
        value = jnp.sum(jnp.where(chosen, gates[...].astype(F32), 0.0), axis=0, keepdims=True)
        named = jnp.broadcast_to(named, (8, n_tokens))
        rank = jnp.dot(named.astype(BF16), before, preferred_element_type=F32)
        picked = jnp.where((named > 0.5) & (jnp.abs(rank - ranks) < 0.5), 1.0, 0.0)
        return picked, jnp.broadcast_to(value, (8, n_tokens))

    picked, _ = picked_by(me_e)
    selected = jnp.dot(picked.astype(BF16), tokens[...], preferred_element_type=F32)
    rows_all[0] = selected[:CAP].astype(BF16)

    pl.semaphore_wait(barrier, n_expert * n_group - 1)

    x_copies, rows_copies = {}, {}
    for s in order[1:]:
        x_copies[s] = pltpu.make_async_remote_copy(
            src_ref=tokens.at[:, own_columns], dst_ref=x_all.at[s],
            send_sem=x_send.at[s], recv_sem=x_recv.at[s],
            device_id={"group": group_at(s)}, device_id_type=MESH,
        )
        x_copies[s].start()
    for s in order[1:]:
        rows_copies[s] = pltpu.make_async_remote_copy(
            src_ref=rows_all.at[0], dst_ref=rows_all.at[s],
            send_sem=rows_send.at[s], recv_sem=rows_recv.at[s],
            device_id={"group": group_at(s)}, device_id_type=MESH,
        )
        rows_copies[s].start()

    feature = lax.broadcasted_iota(jnp.int32, (LANES, 4 * LANES), 0)
    place = lax.broadcasted_iota(jnp.int32, (LANES, 4 * LANES), 1)
    spread = (
        (place == 2 * feature) | (place == 2 * feature + 1 + 2 * LANES)
    ).astype(BF16)

    def project(x, weights, groups, wait):
        depth = min(DEPTH, x.shape[1])
        totals = [None] * (tiles // pair)
        for n in range(x.shape[1] // depth):
            if wait:
                for copy in groups[n]:
                    copy.wait()
            rows = pl.ds(n * depth, depth)
            x_part = x[:, n * depth : (n + 1) * depth]
            for p in range(tiles // pair):
                block = [weights[p * pair + i, rows] for i in range(pair)]
                block = jnp.concatenate(block, axis=1) if pair > 1 else block[0]
                product = jnp.dot(x_part, block, preferred_element_type=F32)
                totals[p] = product if totals[p] is None else totals[p] + product
        return totals

    pre_copies = []
    for b, members in enumerate(batches):
        for s in members:
            if s:
                x_copies[s].wait_recv()
            else:
                own_copy.wait()

        def expand(j, carry, members=members):
            source = pl.ds(pl.multiple_of(j * LANES, LANES), LANES)
            target = pl.ds(pl.multiple_of(j * 2 * LANES, 2 * LANES), 2 * LANES)
            part = jnp.concatenate([x_all[s, :, source] for s in members], axis=0)
            both = jnp.dot(part, spread, preferred_element_type=F32).astype(BF16)
            x_shared[:n_rows, target] = both[:, : 2 * LANES]
            x_shared[n_rows:, target] = both[:, 2 * LANES :]
            return carry

        lax.fori_loop(0, columns // LANES, expand, 0, unroll=True)
        for p, total in enumerate(project(x_shared, w_shared, shared_groups, b == 0)):
            at = pl.ds(p * pair * LANES, pair * LANES)
            pre_own[b, :, at] = total
            pre_out[b, :, at] = total.astype(BF16)
        copies = []
        for d in range(1, n_expert):
            copy = pltpu.make_async_remote_copy(
                src_ref=pre_out.at[b], dst_ref=pre_in.at[d - 1, b],
                send_sem=pre_send.at[d - 1, b], recv_sem=pre_recv.at[d - 1, b],
                device_id={"expert": expert_at(d)}, device_id_type=MESH,
            )
            copy.start()
            copies.append(copy)
        pre_copies.append(copies)

    term_copies = {}
    piece = columns // 7 if columns % (7 * LANES) == 0 else columns
    for b, members in enumerate(batches):
        for copy in pre_copies[b]:
            copy.wait_recv()
        total = pre_own[b]
        for d in range(1, n_expert):
            total = total + pre_in[d - 1, b].astype(F32)
        hidden = (silu(total[:n_rows]) * total[n_rows:]).astype(BF16)
        if b == 0:
            for copy in shared_down_copies:
                copy.wait()
        for n in range(columns // piece):
            at = pl.ds(n * piece, piece)
            term = jnp.dot(hidden, w_shared_down[:, at], preferred_element_type=F32).astype(BF16)
            for i, s in enumerate(members):
                rows = term[i * n_tokens : (i + 1) * n_tokens]
                if s:
                    term_out[s, :, at] = rows
                else:
                    term_in[0, :, at] = rows
        for s in members:
            if s:
                term_copies[s] = pltpu.make_async_remote_copy(
                    src_ref=term_out.at[s], dst_ref=term_in.at[s],
                    send_sem=term_send.at[s], recv_sem=term_recv.at[s],
                    device_id={"group": group_at(-s)}, device_id_type=MESH,
                )
                term_copies[s].start()

    for s in order[1:]:
        rows_copies[s].wait_recv()
    routed_rows = n_group * CAP

    def expand_rows(j, carry):
        source = pl.ds(pl.multiple_of(j * LANES, LANES), LANES)
        target = pl.ds(pl.multiple_of(j * 2 * LANES, 2 * LANES), 2 * LANES)
        part = rows_all[:, :, source].reshape(routed_rows, LANES)
        both = jnp.dot(part, spread, preferred_element_type=F32).astype(BF16)
        x_routed[:routed_rows, target] = both[:, : 2 * LANES]
        x_routed[routed_rows:, target] = both[:, 2 * LANES :]
        return carry

    lax.fori_loop(0, width // LANES, expand_rows, 0, unroll=True)
    totals = project(x_routed, w_routed, routed_groups, True)
    hidden = jnp.concatenate(
        [(silu(t[:routed_rows]) * t[routed_rows:]).astype(BF16) for t in totals], axis=1
    )
    routed_copies = {}
    for d in reversed(range(n_expert)):
        down_copies[d].wait()
        for n in range(columns // piece):
            at = pl.ds(n * piece, piece)
            term = jnp.dot(hidden, w_down[d, :, at], preferred_element_type=F32).astype(BF16)
            for s in range(n_group):
                rows = term[s * CAP : (s + 1) * CAP]
                if d or s:
                    routed_out[d, s, :, at] = rows
                else:
                    routed_in[0, 0, :, at] = rows
        for s in order:
            if d or s:
                routed_copies[d, s] = pltpu.make_async_remote_copy(
                    src_ref=routed_out.at[d, s], dst_ref=routed_in.at[d, s],
                    send_sem=routed_send.at[d, s], recv_sem=routed_recv.at[d, s],
                    device_id={"expert": expert_at(-d), "group": group_at(-s)},
                    device_id_type=MESH,
                )
                routed_copies[d, s].start()

    identity = (
        lax.broadcasted_iota(jnp.int32, (n_tokens, n_tokens), 0)
        == lax.broadcasted_iota(jnp.int32, (n_tokens, n_tokens), 1)
    ).astype(BF16)
    weights = []
    for d in range(n_expert):
        picked, value = picked_by(expert_at(d))
        weights.append(lax.dot_general(
            identity, (picked * value).astype(BF16), (((1,), (1,)), ((), ())),
            preferred_element_type=F32,
        ))
    for s in order[1:]:
        term_copies[s].wait_recv()
    for copy in routed_copies.values():
        copy.wait_recv()
    for n in range(columns // piece):
        at = pl.ds(n * piece, piece)
        total = term_in[0, :, at].astype(F32)
        for s in order[1:]:
            total = total + term_in[s, :, at].astype(F32)
        for d in range(n_expert):
            rows = routed_in[d, 0, :, at].astype(F32)
            for s in range(1, n_group):
                rows = rows + routed_in[d, s, :, at].astype(F32)
            for r in range(CAP):
                total = total + weights[d][:, r : r + 1] * rows[r : r + 1]
        out[:, at] = total.astype(BF16)

    for copies in (x_copies, rows_copies, term_copies, routed_copies):
        for copy in copies.values():
            copy.wait_send()
    for copies in pre_copies:
        for copy in copies:
            copy.wait_send()


def per_device(n_expert, n_group, tokens, ids, gates, gate_up, down, shared_gate_up, shared_down):
    n_tokens, width = tokens.shape
    columns, _, units = shared_gate_up.shape
    tiles = units // LANES
    batch = 2 if n_group % 2 == 0 else 1
    n_batches = n_group // batch
    n_rows = batch * n_tokens
    vmem, dma = pltpu.VMEM, pltpu.SemaphoreType.DMA
    in_vmem, in_hbm = pl.BlockSpec(memory_space=pltpu.VMEM), pl.BlockSpec(memory_space=pltpu.HBM)
    return pl.pallas_call(
        functools.partial(kernel, n_expert, n_group, batch),
        out_shape=jax.ShapeDtypeStruct((n_tokens, columns), BF16),
        in_specs=[in_vmem] * 3 + [in_hbm] * 4,
        out_specs=in_vmem,
        scratch_shapes=[
            vmem((tiles, 2 * width, LANES), BF16),
            vmem((n_expert, units, columns), BF16),
            vmem((tiles, 2 * columns, LANES), BF16),
            vmem((units, columns), BF16),
            vmem((n_group, n_tokens, columns), BF16),
            vmem((2 * n_rows, 2 * columns), BF16),
            vmem((n_group, CAP, width), BF16),
            vmem((2 * n_group * CAP, 2 * width), BF16),
            vmem((n_batches, 2 * n_rows, units), F32),
            vmem((n_batches, 2 * n_rows, units), BF16),
            vmem((max(1, n_expert - 1), n_batches, 2 * n_rows, units), BF16),
            vmem((n_group, n_tokens, columns), BF16),
            vmem((n_group, n_tokens, columns), BF16),
            vmem((n_expert, n_group, CAP, columns), BF16),
            vmem((n_expert, n_group, CAP, columns), BF16),
            dma((max(1, 2 * width // DEPTH), tiles)),
            dma((n_expert,)),
            dma((max(1, 2 * columns // DEPTH), tiles)),
            dma((4,)),
            dma,
            dma((n_group,)), dma((n_group,)),
            dma((n_group,)), dma((n_group,)),
            dma((max(1, n_expert - 1), n_batches)), dma((max(1, n_expert - 1), n_batches)),
            dma((n_group,)), dma((n_group,)),
            dma((n_expert, n_group)), dma((n_expert, n_group)),
        ],
        compiler_params=pltpu.CompilerParams(
            collective_id=0, has_side_effects=True, vmem_limit_bytes=60 * 2**20
        ),
    )(tokens, ids.T, gates.T, gate_up, down, shared_gate_up, shared_down)


def solution(mesh):
    in_specs = (
        P(("dp", "group"), None),
        P(("dp", "group"), None),
        P(("dp", "group"), None),
        P("expert", None, None, "group"),
        P("expert", "group", None),
        P("expert", None, "group"),
        P("group", "expert"),
    )
    return jax.shard_map(
        functools.partial(per_device, mesh.shape["expert"], mesh.shape["group"]),
        mesh=mesh, in_specs=in_specs, out_specs=P(("dp", "group"), "expert"), check_vma=False,
    )
```

```python
import functools

import jax
import jax.numpy as jnp
from jax import lax
from jax.experimental import pallas as pl
from jax.experimental.pallas import tpu as pltpu
from jax.sharding import PartitionSpec as P

MESH = pl.DeviceIdType.MESH
BF16, F32 = jnp.bfloat16, jnp.float32
CAP = 2
LANES = 128
DEPTH = 1792


def nearest_first(count):
    order = []
    for distance in range(1, count // 2 + 1):
        for candidate in (distance, count - distance):
            if candidate not in order:
                order.append(candidate)
    return order


def batches_of(count):
    order = nearest_first(count) + [0]
    return [order[i : i + 2] for i in range(0, count, 2)]


def schedule_of(batches):
    return [(kind, b) for kind in ("pre", "fin") for b in range(len(batches))]


def silu(value):
    return value / (1.0 + jnp.exp(-value))


def kernel(
    n_expert, n_group,
    tokens, ids, gates, gate_up, down, shared_gate_up, shared_down,
    out,
    w_routed, w_down, w_shared, w_shared_down,
    x_all, x_shared, rows_all, x_routed,
    pre_own, pre_out, pre_in, term_out, term_in, routed_out, routed_in,
    routed_w_sem, down_w_sem, shared_w_sem, shared_down_w_sem, own_sem,
    x_send, x_recv, rows_send, rows_recv, pre_send, pre_recv,
    term_send, term_recv, routed_send, routed_recv,
):
    me_e, me_g = lax.axis_index("expert"), lax.axis_index("group")
    n_tokens, width = tokens.shape
    columns = x_all.shape[2]
    units = w_shared_down.shape[0]
    tiles = units // LANES
    pair = 2 if tiles % 2 == 0 else 1
    order = nearest_first(n_group)
    batches = batches_of(n_group)

    def expert_at(distance):
        return lax.rem(me_e + n_expert + distance, n_expert)

    def group_at(distance):
        return lax.rem(me_g + n_group + distance, n_group)

    def weight_copies(source, target, sem):
        depth = min(DEPTH, source.shape[0])
        groups = []
        for n in range(source.shape[0] // depth):
            rows = pl.ds(n * depth, depth)
            groups.append([
                pltpu.make_async_copy(
                    source.at[rows, pl.ds(c * LANES, LANES)], target.at[c, rows], sem.at[n, c]
                )
                for c in range(tiles)
            ])
        return groups

    shared_groups = weight_copies(
        shared_gate_up.reshape(2 * columns, units), w_shared, shared_w_sem
    )
    routed_groups = weight_copies(gate_up.reshape(2 * width, units), w_routed, routed_w_sem)
    part = units // 4
    shared_down_copies = [
        pltpu.make_async_copy(
            shared_down.at[pl.ds(i * part, part)], w_shared_down.at[pl.ds(i * part, part)],
            shared_down_w_sem.at[i],
        )
        for i in range(4)
    ]
    down_copies = [
        pltpu.make_async_copy(
            down.at[0, :, pl.ds(pl.multiple_of(expert_at(-d) * columns, LANES), columns)],
            w_down.at[d],
            down_w_sem.at[d],
        )
        for d in range(n_expert)
    ]
    own_columns = pl.ds(pl.multiple_of(me_e * columns, LANES), columns)
    own_copy = pltpu.make_async_copy(tokens.at[:, own_columns], x_all.at[0], own_sem)
    own_copy.start()
    for group in shared_groups:
        for copy in group:
            copy.start()
    for copy in shared_down_copies:
        copy.start()
    for group in routed_groups:
        for copy in group:
            copy.start()
    for copy in down_copies:
        copy.start()

    barrier = pltpu.get_barrier_semaphore()
    for d in range(n_expert):
        for s in range(n_group):
            if d or s:
                pl.semaphore_signal(
                    barrier, inc=1,
                    device_id={"expert": expert_at(d), "group": group_at(s)},
                    device_id_type=MESH,
                )

    before = (
        lax.broadcasted_iota(jnp.int32, (n_tokens, n_tokens), 0)
        < lax.broadcasted_iota(jnp.int32, (n_tokens, n_tokens), 1)
    ).astype(BF16)
    ranks = lax.broadcasted_iota(jnp.int32, (8, n_tokens), 0).astype(F32)

    def picked_by(expert):
        chosen = ids[...] == expert
        named = jnp.sum(jnp.where(chosen, 1.0, 0.0), axis=0, keepdims=True)
        value = jnp.sum(jnp.where(chosen, gates[...].astype(F32), 0.0), axis=0, keepdims=True)
        named = jnp.broadcast_to(named, (8, n_tokens))
        rank = jnp.dot(named.astype(BF16), before, preferred_element_type=F32)
        picked = jnp.where((named > 0.5) & (jnp.abs(rank - ranks) < 0.5), 1.0, 0.0)
        return picked, jnp.broadcast_to(value, (8, n_tokens))

    picked, _ = picked_by(me_e)
    selected = jnp.dot(picked.astype(BF16), tokens[...], preferred_element_type=F32)
    rows_all[0] = selected[:CAP].astype(BF16)

    pl.semaphore_wait(barrier, n_expert * n_group - 1)

    x_copies, rows_copies = {}, {}
    relayed = n_group == 4
    for s in [1, 3] if relayed else order:
        x_copies[s] = pltpu.make_async_remote_copy(
            src_ref=tokens.at[:, own_columns], dst_ref=x_all.at[s],
            send_sem=x_send.at[s], recv_sem=x_recv.at[s],
            device_id={"group": group_at(s)}, device_id_type=MESH,
        )
        x_copies[s].start()
    x_arrivals = {s: [copy] for s, copy in x_copies.items()}
    if relayed:
        half = columns // 2
        for s, sem, first in ((1, 2, 0), (3, 0, half)):
            x_copies[s].wait_recv()
            at = pl.ds(first, half)
            relay = pltpu.make_async_remote_copy(
                src_ref=x_all.at[s, :, at], dst_ref=x_all.at[2, :, at],
                send_sem=x_send.at[sem], recv_sem=x_recv.at[sem],
                device_id={"group": group_at(s)}, device_id_type=MESH,
            )
            relay.start()
            x_arrivals[s] = []
            x_arrivals.setdefault(2, []).append(relay)
            x_copies["relay", s] = relay
    for s in order:
        rows_copies[s] = pltpu.make_async_remote_copy(
            src_ref=rows_all.at[0], dst_ref=rows_all.at[s],
            send_sem=rows_send.at[s], recv_sem=rows_recv.at[s],
            device_id={"group": group_at(s)}, device_id_type=MESH,
        )
        rows_copies[s].start()

    feature = lax.broadcasted_iota(jnp.int32, (LANES, 4 * LANES), 0)
    place = lax.broadcasted_iota(jnp.int32, (LANES, 4 * LANES), 1)
    spread = (
        (place == 2 * feature) | (place == 2 * feature + 1 + 2 * LANES)
    ).astype(BF16)

    def project(x, weights, groups, wait):
        depth = min(DEPTH, x.shape[1])
        totals = [None] * (tiles // pair)
        for n in range(x.shape[1] // depth):
            if wait:
                for copy in groups[n]:
                    copy.wait()
            rows = pl.ds(n * depth, depth)
            x_part = x[:, pl.ds(n * depth, depth)]
            for p in range(tiles // pair):
                block = [weights[p * pair + i, rows] for i in range(pair)]
                block = jnp.concatenate(block, axis=1) if pair > 1 else block[0]
                product = jnp.dot(x_part, block, preferred_element_type=F32)
                totals[p] = product if totals[p] is None else totals[p] + product
        return totals

    pre_copies, term_copies = {}, {}
    piece = columns // 7 if columns % (7 * LANES) == 0 else columns
    shared_waits = list(shared_groups)

    def pre(b):
        members = batches[b]
        n_rows = len(members) * n_tokens
        for s in members:
            if s:
                for copy in x_arrivals[s]:
                    copy.wait_recv()
            else:
                own_copy.wait()

        def expand(j, carry):
            source = pl.ds(pl.multiple_of(j * LANES, LANES), LANES)
            target = pl.ds(pl.multiple_of(j * 2 * LANES, 2 * LANES), 2 * LANES)
            part = jnp.concatenate([x_all[s, :, source] for s in members], axis=0)
            both = jnp.dot(part, spread, preferred_element_type=F32).astype(BF16)
            x_shared[:n_rows, target] = both[:, : 2 * LANES]
            x_shared[n_rows : 2 * n_rows, target] = both[:, 2 * LANES :]
            return carry

        lax.fori_loop(0, columns // LANES, expand, 0, unroll=True)
        totals = project(x_shared.at[: 2 * n_rows], w_shared, shared_groups, bool(shared_waits))
        shared_waits.clear()
        for p, total in enumerate(totals):
            at = pl.ds(p * pair * LANES, pair * LANES)
            pre_own[b, : 2 * n_rows, at] = total
            pre_out[b, : 2 * n_rows, at] = total.astype(BF16)
        pre_copies[b] = []
        for d in range(1, n_expert):
            rows = pl.ds(0, 2 * n_rows)
            copy = pltpu.make_async_remote_copy(
                src_ref=pre_out.at[b, rows], dst_ref=pre_in.at[d - 1, b, rows],
                send_sem=pre_send.at[d - 1, b], recv_sem=pre_recv.at[d - 1, b],
                device_id={"expert": expert_at(d)}, device_id_type=MESH,
            )
            copy.start()
            pre_copies[b].append(copy)

    down_waits = list(shared_down_copies)

    def fin(b):
        members = batches[b]
        n_rows = len(members) * n_tokens
        for copy in pre_copies[b]:
            copy.wait_recv()
        total = pre_own[b, : 2 * n_rows]
        for d in range(1, n_expert):
            total = total + pre_in[d - 1, b, : 2 * n_rows].astype(F32)
        hidden = (silu(total[:n_rows]) * total[n_rows:]).astype(BF16)
        for copy in down_waits:
            copy.wait()
        down_waits.clear()
        for n in range(columns // piece):
            at = pl.ds(n * piece, piece)
            term = jnp.dot(hidden, w_shared_down[:, at], preferred_element_type=F32).astype(BF16)
            for i, s in enumerate(members):
                rows = term[i * n_tokens : (i + 1) * n_tokens]
                if s:
                    term_out[s, :, at] = rows
                else:
                    term_in[0, :, at] = rows
        for s in members:
            if s:
                term_copies[s] = pltpu.make_async_remote_copy(
                    src_ref=term_out.at[s], dst_ref=term_in.at[s],
                    send_sem=term_send.at[s], recv_sem=term_recv.at[s],
                    device_id={"group": group_at(-s)}, device_id_type=MESH,
                )
                term_copies[s].start()

    for kind, b in schedule_of(batches):
        (pre if kind == "pre" else fin)(b)

    for s in order:
        rows_copies[s].wait_recv()
    routed_rows = n_group * CAP

    def expand_rows(j, carry):
        source = pl.ds(pl.multiple_of(j * LANES, LANES), LANES)
        target = pl.ds(pl.multiple_of(j * 2 * LANES, 2 * LANES), 2 * LANES)
        part = rows_all[:, :, source].reshape(routed_rows, LANES)
        both = jnp.dot(part, spread, preferred_element_type=F32).astype(BF16)
        x_routed[:routed_rows, target] = both[:, : 2 * LANES]
        x_routed[routed_rows:, target] = both[:, 2 * LANES :]
        return carry

    lax.fori_loop(0, width // LANES, expand_rows, 0, unroll=True)
    totals = project(x_routed, w_routed, routed_groups, True)
    hidden = jnp.concatenate(
        [(silu(t[:routed_rows]) * t[routed_rows:]).astype(BF16) for t in totals], axis=1
    )
    routed_copies = {}
    for d in reversed(range(n_expert)):
        down_copies[d].wait()
        for n in range(columns // piece):
            at = pl.ds(n * piece, piece)
            term = jnp.dot(hidden, w_down[d, :, at], preferred_element_type=F32).astype(BF16)
            for s in range(n_group):
                rows = term[s * CAP : (s + 1) * CAP]
                if d or s:
                    routed_out[d, s, :, at] = rows
                else:
                    routed_in[0, 0, :, at] = rows
        for s in order + [0]:
            if d or s:
                routed_copies[d, s] = pltpu.make_async_remote_copy(
                    src_ref=routed_out.at[d, s], dst_ref=routed_in.at[d, s],
                    send_sem=routed_send.at[d, s], recv_sem=routed_recv.at[d, s],
                    device_id={"expert": expert_at(-d), "group": group_at(-s)},
                    device_id_type=MESH,
                )
                routed_copies[d, s].start()

    identity = (
        lax.broadcasted_iota(jnp.int32, (n_tokens, n_tokens), 0)
        == lax.broadcasted_iota(jnp.int32, (n_tokens, n_tokens), 1)
    ).astype(BF16)
    weights = []
    for d in range(n_expert):
        picked, value = picked_by(expert_at(d))
        weights.append(lax.dot_general(
            identity, (picked * value).astype(BF16), (((1,), (1,)), ((), ())),
            preferred_element_type=F32,
        ))
    for s in order:
        term_copies[s].wait_recv()
    for copy in routed_copies.values():
        copy.wait_recv()
    for n in range(columns // piece):
        at = pl.ds(n * piece, piece)
        total = term_in[0, :, at].astype(F32)
        for s in order:
            total = total + term_in[s, :, at].astype(F32)
        for d in range(n_expert):
            rows = routed_in[d, 0, :, at].astype(F32)
            for s in range(1, n_group):
                rows = rows + routed_in[d, s, :, at].astype(F32)
            for r in range(CAP):
                total = total + weights[d][:, r : r + 1] * rows[r : r + 1]
        out[:, at] = total.astype(BF16)

    for copies in (x_copies, rows_copies, term_copies, routed_copies):
        for copy in copies.values():
            copy.wait_send()
    for copies in pre_copies.values():
        for copy in copies:
            copy.wait_send()


def per_device(n_expert, n_group, tokens, ids, gates, gate_up, down, shared_gate_up, shared_down):
    n_tokens, width = tokens.shape
    columns, _, units = shared_gate_up.shape
    tiles = units // LANES
    batches = batches_of(n_group)
    n_batches = len(batches)
    n_rows = max(len(members) for members in batches) * n_tokens
    vmem, dma = pltpu.VMEM, pltpu.SemaphoreType.DMA
    in_vmem, in_hbm = pl.BlockSpec(memory_space=pltpu.VMEM), pl.BlockSpec(memory_space=pltpu.HBM)
    return pl.pallas_call(
        functools.partial(kernel, n_expert, n_group),
        out_shape=jax.ShapeDtypeStruct((n_tokens, columns), BF16),
        in_specs=[in_vmem] * 3 + [in_hbm] * 4,
        out_specs=in_vmem,
        scratch_shapes=[
            vmem((tiles, 2 * width, LANES), BF16),
            vmem((n_expert, units, columns), BF16),
            vmem((tiles, 2 * columns, LANES), BF16),
            vmem((units, columns), BF16),
            vmem((n_group, n_tokens, columns), BF16),
            vmem((2 * n_rows, 2 * columns), BF16),
            vmem((n_group, CAP, width), BF16),
            vmem((2 * n_group * CAP, 2 * width), BF16),
            vmem((n_batches, 2 * n_rows, units), F32),
            vmem((n_batches, 2 * n_rows, units), BF16),
            vmem((max(1, n_expert - 1), n_batches, 2 * n_rows, units), BF16),
            vmem((n_group, n_tokens, columns), BF16),
            vmem((n_group, n_tokens, columns), BF16),
            vmem((n_expert, n_group, CAP, columns), BF16),
            vmem((n_expert, n_group, CAP, columns), BF16),
            dma((max(1, 2 * width // DEPTH), tiles)),
            dma((n_expert,)),
            dma((max(1, 2 * columns // DEPTH), tiles)),
            dma((4,)),
            dma,
            dma((n_group,)), dma((n_group,)),
            dma((n_group,)), dma((n_group,)),
            dma((max(1, n_expert - 1), n_batches)), dma((max(1, n_expert - 1), n_batches)),
            dma((n_group,)), dma((n_group,)),
            dma((n_expert, n_group)), dma((n_expert, n_group)),
        ],
        compiler_params=pltpu.CompilerParams(
            collective_id=0, has_side_effects=True, vmem_limit_bytes=60 * 2**20
        ),
    )(tokens, ids.T, gates.T, gate_up, down, shared_gate_up, shared_down)


def solution(mesh):
    in_specs = (
        P(("dp", "group"), None),
        P(("dp", "group"), None),
        P(("dp", "group"), None),
        P("expert", None, None, "group"),
        P("expert", "group", None),
        P("expert", None, "group"),
        P("group", "expert"),
    )
    return jax.shard_map(
        functools.partial(per_device, mesh.shape["expert"], mesh.shape["group"]),
        mesh=mesh, in_specs=in_specs, out_specs=P(("dp", "group"), "expert"), check_vma=False,
    )
```
